32 devices in a mesh: group: 4 (over y, x), shard: 8 (over z, core).
Axes of the slice: x: 2, y: 2, z: 4, core: 2. Of those that a mesh axis runs over, the one named last changes fastest.
Arguments:
- grad_pooled: bfloat16 [4096, 512, 128], P(('group', 'shard')), may hold values from -6 to 6
- bag_rows: int32 [4096, 512, 8], P(('group', 'shard')), may hold values from 0 to 511
- bag_lengths: int32 [4096, 512], P(('group', 'shard')), may hold values from 1 to 8
- table_order: int32 [512], replicated, may hold values from 0 to 511, each once
- weights: bfloat16 [512, 512, 128], P('shard'), may hold values from -6 to 6
- accum: float32 [512, 512], P('shard'), may hold values from 0.1 to 10
Outputs:
- new_weights: bfloat16 [512, 512, 128], P('shard')
- new_accum: float32 [512, 512], P('shard')
The draws below stay inside these ranges and needn't reach their ends.
All inputs are finite; a program needn't handle non-finite values.
Results may differ from the reference program's by a relative error of at most 0.001.
Values may be sent and summed in bfloat16 or wider, within the bound.
A program may use at most 128 MiB of HBM per device.

```python
import math
import jax
import jax.numpy as jnp
from jax import lax

D = 128
TABLES = 512
ROWS = 512
BAG = 8
BATCH = 4096


def plant(values, own_key, smallest, high):
    longest = values.shape.index(max(values.shape))
    spots = []
    for shift in (0, 1):
        where = [jax.random.randint(jax.random.fold_in(own_key, axis), (), 0, length) for axis, length in enumerate(values.shape)]
        where[longest] = (where[longest] + shift) % values.shape[longest]
        spots.append(tuple(where))
    return values.at[spots[0]].set(smallest).at[spots[1]].set(high)


def steps_of(rng, dims, cuts, least, top_value):
    gain, own = 1.0, jax.random.fold_in(rng, 6)
    for axis_at, blocks in cuts:
        heights = jnp.exp(jax.random.uniform(jax.random.fold_in(own, axis_at), (blocks,), jnp.float32, least / len(cuts), top_value / len(cuts)))
        gain = gain * jnp.repeat(heights, dims[axis_at] // blocks).reshape([-1 if axis == axis_at else 1 for axis in range(len(dims))])
    return gain


def noise(own_key, shape, scale, reach, split=(), kind=jnp.bfloat16):
    level = steps_of(own_key, shape, split, -0.22, 0.18) if split else 1.0
    entries = jax.random.normal(own_key, shape, jnp.float32) * scale * level
    return jnp.minimum(jnp.maximum(entries, -reach), reach).astype(kind)


def setup_inputs(seed: int = 0) -> dict:
    seeds = jax.random.split(jax.random.key(seed), 7)
    grad_pooled = noise(seeds[0], (BATCH, TABLES, D), 1.0, 6.0, ((0, 32),))
    bag_rows = plant(jax.random.randint(seeds[1], (BATCH, TABLES, BAG), 0, ROWS), jax.random.fold_in(seeds[1], 1), 0, ROWS - 1).astype(jnp.int32)
    bag_lengths = plant(jax.random.randint(seeds[2], (BATCH, TABLES), 1, BAG + 1), jax.random.fold_in(seeds[2], 1), 1, BAG).astype(jnp.int32)
    table_order = jax.random.permutation(seeds[3], TABLES).astype(jnp.int32)
    weights = noise(seeds[4], (TABLES, ROWS, D), 1.0, 6.0, ((0, 8),))
    accum = jnp.clip(jnp.exp(math.log(10.0) - 4.6051702 * jax.random.uniform(seeds[5], (TABLES, ROWS), jnp.float32) ** steps_of(seeds[5], (TABLES, ROWS), ((0, 8),), -0.2, 0.2)), 0.1, 10.0)
    return dict(grad_pooled=grad_pooled, bag_rows=bag_rows, bag_lengths=bag_lengths, table_order=table_order, weights=weights, accum=accum)


LEARN_RATE = 0.5
EPSILON = 1e-06

def reference(grad_pooled, bag_rows, bag_lengths, table_order, weights, accum):
    pooled = jnp.take(grad_pooled, table_order, axis=1).astype(jnp.float32)
    places = jnp.arange(BAG, dtype=jnp.int32)
    live = places[None, None, :] < bag_lengths[:, :, None]
    row_ids = jnp.where(live, bag_rows, ROWS).astype(jnp.int32)
    row_ids = jnp.take(row_ids, table_order, axis=1)

    def one_table(member):
        values, chosen = member
        spread = jnp.broadcast_to(values[:, None, :], (values.shape[0], BAG, D)).reshape(-1, D)
        summed = jax.ops.segment_sum(spread, chosen.reshape(-1), num_segments=ROWS + 1)
        return summed[:ROWS]
    row_grad = lax.map(one_table, (jnp.swapaxes(pooled, 0, 1), jnp.swapaxes(row_ids, 0, 1)))
    new_accum = accum + lax.optimization_barrier(jnp.mean(row_grad * row_grad, axis=-1))
    step_size = LEARN_RATE / (jnp.sqrt(new_accum) + EPSILON)
    new_weights = (weights.astype(jnp.float32) - step_size[:, :, None] * row_grad).astype(jnp.bfloat16)
    return (new_weights, new_accum)
```

```python
import functools

import jax
import jax.numpy as jnp
from jax import lax
from jax.experimental import pallas as pl
from jax.experimental.pallas import tpu as pltpu
from jax.sharding import PartitionSpec as P

LEARN_RATE = 0.5
EPSILON = 1e-06
AXES = ("group", "shard")
CHUNKS = 4
TILE = 16


def arrange_kernel(order_ref, grad_ref, *rest):
    *outs, flipped = rest
    tables = grad_ref.shape[1]
    part = outs[0].shape[0]

    def flip(step, carry):
        start = pl.multiple_of(step * TILE, TILE)
        block = grad_ref[:, pl.ds(start, TILE), :]
        flipped[pl.ds(start, TILE)] = jnp.swapaxes(block, 0, 1)
        return carry

    lax.fori_loop(0, tables // TILE, flip, 0)
    for chunk, out in enumerate(outs):

        def place(step, carry, chunk=chunk, out=out):
            for k in range(8):
                at = step * 8 + k
                out[at] = flipped[order_ref[chunk * part + at]]
            return carry

        lax.fori_loop(0, part // 8, place, 0)


def arrange(grad_pooled, order, chunks):
    samples, tables, width = grad_pooled.shape
    part = tables // chunks
    return pl.pallas_call(
        arrange_kernel,
        grid_spec=pltpu.PrefetchScalarGridSpec(
            num_scalar_prefetch=1,
            grid=(samples // TILE,),
            in_specs=[pl.BlockSpec((TILE, tables, width), lambda b, order: (b, 0, 0))],
            out_specs=[
                pl.BlockSpec((part, TILE, width), lambda b, order: (0, b, 0))
                for _ in range(chunks)
            ],
            scratch_shapes=[pltpu.VMEM((tables, TILE, width), grad_pooled.dtype)],
        ),
        out_shape=[
            jax.ShapeDtypeStruct((part, samples, width), grad_pooled.dtype)
            for _ in range(chunks)
        ],
        cost_estimate=pl.CostEstimate(
            flops=0, bytes_accessed=4 * grad_pooled.size, transcendentals=0
        ),
    )(order, grad_pooled)


def expand_kernel(offset, unroll, rows_ref, grad_ref, out_ref, counts):
    sources, _, bag, samples = rows_ref.shape
    row_count = out_ref.shape[1]
    place = lax.broadcasted_iota(jnp.int32, (TILE, samples), 0).astype(jnp.float32)
    places = [(place + float(r * TILE - offset)).astype(jnp.bfloat16) for r in range(row_count // TILE)]
    one = jnp.ones((TILE, samples), jnp.bfloat16)
    zero = jnp.zeros((TILE, samples), jnp.bfloat16)
    out_ref[...] = jnp.zeros_like(out_ref)

    def step(i, carry):
        for u in range(unroll):
            picks = rows_ref[i * unroll + u, 0].astype(jnp.float32)
            spread = [
                jnp.broadcast_to(picks[j : j + 1], (TILE, samples)).astype(jnp.bfloat16)
                for j in range(bag)
            ]
            for r, here in enumerate(places):
                terms = [jnp.where(s == here, one, zero) for s in spread]
                while len(terms) > 1:
                    terms = [a + b for a, b in zip(terms[::2], terms[1::2])] + (
                        [terms[-1]] if len(terms) % 2 else []
                    )
                counts[r * TILE : (r + 1) * TILE, u * samples : (u + 1) * samples] = terms[0]
        values = grad_ref[pl.ds(i * unroll, unroll), 0].reshape(unroll * samples, -1)
        out_ref[0] += jnp.dot(counts[...], values, preferred_element_type=jnp.float32)
        return carry

    lax.fori_loop(0, sources // unroll, step, 0)


def expand_rows(gradient, row_ids, first, row_count, offset):
    sources, tables, samples, width = gradient.shape
    bag = row_ids.shape[2]
    unroll = 4 if sources % 4 == 0 else 1
    return pl.pallas_call(
        functools.partial(expand_kernel, offset, unroll),
        grid=(tables,),
        in_specs=[
            pl.BlockSpec((sources, 1, bag, samples), lambda t: (0, first + t, 0, 0)),
            pl.BlockSpec((sources, 1, samples, width), lambda t: (0, t, 0, 0)),
        ],
        out_specs=pl.BlockSpec((1, row_count, width), lambda t: (t, 0, 0)),
        out_shape=jax.ShapeDtypeStruct((tables, row_count, width), jnp.float32),
        scratch_shapes=[pltpu.VMEM((row_count, unroll * samples), jnp.bfloat16)],
        cost_estimate=pl.CostEstimate(
            flops=40 * gradient.size * row_count // 8,
            bytes_accessed=2 * gradient.size,
            transcendentals=0,
        ),
    )(row_ids, gradient)


def body(grad_pooled, bag_rows, bag_lengths, table_order, weights, accum):
    row_count = weights.shape[1]
    samples, tables, width = grad_pooled.shape
    bag = bag_rows.shape[2]
    groups = lax.axis_size("group")
    shards = lax.axis_size("shard")
    devices = groups * shards
    held = weights.shape[0]
    quarter = held // groups
    chunks = CHUNKS if quarter % CHUNKS == 0 else 1
    each = quarter // chunks
    offset = row_count // 2
    me = lax.axis_index("group")

    by_slot = table_order.reshape(shards, chunks, groups, each)
    by_chunk = by_slot.transpose(1, 2, 0, 3).reshape(-1)
    by_device = by_slot.transpose(2, 0, 1, 3).reshape(-1)

    live = jnp.arange(bag, dtype=jnp.int32)[None, :, None] < bag_lengths[:, None, :]
    ids = jnp.where(live, jnp.transpose(bag_rows, (0, 2, 1)), row_count) - offset
    ids = jnp.transpose(ids.astype(jnp.float32), (2, 1, 0))
    ids = jnp.take(ids, by_device, axis=0, mode="clip", unique_indices=True).astype(jnp.bfloat16)
    ids = lax.all_to_all(ids, AXES, split_axis=0, concat_axis=0, tiled=True)
    ids = ids.reshape(devices, quarter, bag, samples)

    sends = arrange(grad_pooled, by_chunk, chunks)
    received = []
    for chunk in range(chunks):
        send = sends[chunk]
        if received:
            send, received[-1] = lax.optimization_barrier((send, received[-1]))
        received.append(lax.all_to_all(send, AXES, split_axis=0, concat_axis=0, tiled=True))

    weights_by = weights.reshape(chunks, groups, each, row_count, width)
    accum_by = accum.reshape(chunks, groups, each, row_count)
    full_weights, sums = [], []
    for chunk in range(chunks):
        gradient = received[chunk].reshape(devices, each, samples, width)
        row_grad = expand_rows(gradient, ids, chunk * each, row_count, offset)
        weight_part = lax.dynamic_index_in_dim(weights_by[chunk], me, 0, keepdims=False)
        accum_part = lax.dynamic_index_in_dim(accum_by[chunk], me, 0, keepdims=False)
        new_accum = accum_part + jnp.mean(row_grad * row_grad, axis=-1)
        step_size = LEARN_RATE / (jnp.sqrt(new_accum) + EPSILON)
        new_weights = weight_part.astype(jnp.float32) - step_size[:, :, None] * row_grad
        full_weights.append(
            lax.all_gather(new_weights.astype(jnp.bfloat16), "group", axis=0, tiled=True)
        )
        sums.append(new_accum)
    all_sums = lax.all_gather(jnp.stack(sums), "group", axis=1)
    return (
        jnp.concatenate(full_weights, axis=0),
        all_sums.reshape(held, row_count),
    )


def solution(mesh):
    in_specs = (
        P(AXES, None, None),
        P(AXES, None, None),
        P(AXES, None),
        P(),
        P("shard", None, None),
        P("shard", None),
    )
    out_specs = (P("shard", None, None), P("shard", None))
    return jax.shard_map(body, mesh=mesh, in_specs=in_specs, out_specs=out_specs, check_vma=False)
```
